8 devices in a mesh: dp: 2 (over y, z), tp: 4 (over x, core).
Axes of the slice: x: 2, y: 2, z: 1, core: 2. Of those that a mesh axis runs over, the one named last changes fastest.
Arguments:
- x: bfloat16 [2, 1536, 3072], P('dp', 'tp'), parts along dimension 0
- dy: bfloat16 [2, 1536, 3072], P('dp', 'tp'), parts along dimension 0
- wq: bfloat16 [3072, 3072], P(None, 'tp')
- wk: bfloat16 [3072, 1024], P(None, 'tp')
- wv: bfloat16 [3072, 1024], P(None, 'tp')
- wo: bfloat16 [3072, 3072], P('tp')
- w_gate: bfloat16 [3072, 8192], P(None, 'tp')
- w_up: bfloat16 [3072, 8192], P(None, 'tp')
- w_down: bfloat16 [8192, 3072], P('tp')
Outputs:
- output 1: bfloat16 [2, 1536, 3072], P('dp', 'tp'), parts along dimension 0
- output 2: bfloat16 [6144, 3072], P('dp', 'tp'), parts along dimension 0
- output 3: bfloat16 [6144, 1024], P('dp', 'tp'), parts along dimension 0
- output 4: bfloat16 [6144, 1024], P('dp', 'tp'), parts along dimension 0
- output 5: bfloat16 [6144, 3072], P(('dp', 'tp')), parts along dimension 0
- output 6: bfloat16 [6144, 8192], P('dp', 'tp'), parts along dimension 0
- output 7: bfloat16 [6144, 8192], P('dp', 'tp'), parts along dimension 0
- output 8: bfloat16 [16384, 3072], P(('dp', 'tp')), parts along dimension 0
There are 2 independent parts. The reference program is written for one: setup_inputs(seed, part) draws one part's arguments, and reference() takes and returns one part's arrays. A program takes and returns all parts, laid end to end along the dimension named above; an argument that names none is the same for every part.
All inputs are finite; a program needn't handle non-finite values.
Results may differ from the reference program's by a relative error of at most 0.024.
Values are sent between devices in bfloat16 or wider.
A program may use at most 2 GiB of HBM per device.

```python
import jax
import jax.numpy as jnp
from jax import lax

SEQUENCES = 1
TOKENS = 1536
D = 3072
HEADS = 24
KV_HEADS = 8
HEAD = 128
FF = 8192
THETA = 10000
NAMES = ("wq", "wk", "wv", "wo", "w_gate", "w_up", "w_down")
SHAPES = {
    "wq": (D, HEADS * HEAD),
    "wk": (D, KV_HEADS * HEAD),
    "wv": (D, KV_HEADS * HEAD),
    "wo": (HEADS * HEAD, D),
    "w_gate": (D, FF),
    "w_up": (D, FF),
    "w_down": (FF, D),
}


def bump(key, n, height):
    away = (jnp.arange(n, dtype=jnp.int32) - jax.random.randint(key, (), 0, n, jnp.int32)) % n
    return jnp.where(away < n // 8, height, 1.0)


def together(key, own, strength):
    shared = jax.random.normal(key, own.shape[1:], jnp.float32)
    return (own + strength * shared) * lax.rsqrt(1 + strength * strength)


def setup_inputs(seed: int = 0, part: int = 0) -> dict:
    kx, kdy, ka, kb, kz, kf, kh, kl, *kw = jax.random.split(jax.random.key(seed), 8 + len(NAMES))
    kx, kdy, ka, kb = (jax.random.fold_in(k, part) for k in (kx, kdy, ka, kb))
    shape = (SEQUENCES, TOKENS, D)
    much_x, much_dy = jax.random.uniform(kz, (2,), jnp.float32, 0.0, 1.0)
    loud = 2.0 ** jax.random.uniform(jax.random.fold_in(kz, 1), (), jnp.float32, -1.0, 2.0)
    halves = 2.0 ** jax.random.uniform(kl, (2,), jnp.float32, -1.0, 1.0)
    times = {"wq": 1.0, "wk": 1.0, "wv": 2.0, "wo": halves[0], "w_gate": 1.0, "w_up": bump(kh, FF, 4.0), "w_down": halves[1]}
    x = together(ka, jax.random.normal(kx, shape, jnp.float32), much_x) * bump(kf, D, 4.0)
    dy = together(kb, jax.random.normal(kdy, shape, jnp.float32), much_dy)
    drawn = {"x": x.astype(jnp.bfloat16), "dy": (loud * dy * (SEQUENCES * TOKENS) ** -0.5).astype(jnp.bfloat16)}
    for key, name in zip(kw, NAMES, strict=True):
        drawn[name] = (jax.random.normal(key, SHAPES[name], jnp.float32) * SHAPES[name][0] ** -0.5 * times[name]).astype(jnp.bfloat16)
    return drawn


def matmul(a, w):
    return jnp.dot(a, w, preferred_element_type=jnp.float32).astype(jnp.bfloat16)


def normed(h):
    wide = h.astype(jnp.float32)
    scale = lax.rsqrt(jnp.mean(wide**2, -1, keepdims=True) + 1e-6)
    return (wide * scale).astype(jnp.bfloat16)


def turned(t, theta):
    half = t.shape[-1] // 2
    angle = jnp.arange(t.shape[0], dtype=jnp.float32)[:, None] * theta ** (-jnp.arange(half, dtype=jnp.float32) / half)
    cos, sin = jnp.cos(angle)[:, None], jnp.sin(angle)[:, None]
    a, b = t[..., :half].astype(jnp.float32), t[..., half:].astype(jnp.float32)
    return jnp.concatenate([a * cos - b * sin, b * cos + a * sin], -1).astype(jnp.bfloat16)


def seen_by(q, k, v):
    tokens, kv = q.shape[0], k.shape[1]
    q = q.reshape(tokens, kv, -1, q.shape[-1])
    scores = jnp.einsum("tgsd,ugd->gstu", q.astype(jnp.float32), k.astype(jnp.float32)) * q.shape[-1] ** -0.5
    place = jnp.arange(tokens)
    weights = jax.nn.softmax(jnp.where(place[:, None] >= place, scores, -jnp.inf), -1).astype(jnp.bfloat16)
    return jnp.einsum("gstu,ugd->tgsd", weights.astype(jnp.float32), v.astype(jnp.float32)).astype(jnp.bfloat16).reshape(tokens, -1)


def layer(h, w):
    a = normed(h)
    q, k = (turned(matmul(a, w[name]).reshape(h.shape[0], -1, HEAD), THETA) for name in ("wq", "wk"))
    h = h + matmul(seen_by(q, k, matmul(a, w["wv"]).reshape(h.shape[0], -1, HEAD)), w["wo"])
    b = normed(h)
    gate = jnp.dot(b, w["w_gate"], preferred_element_type=jnp.float32)
    up = jnp.dot(b, w["w_up"], preferred_element_type=jnp.float32)
    return h + matmul((jax.nn.silu(gate) * up).astype(jnp.bfloat16), w["w_down"])


def reference(x, dy, wq, wk, wv, wo, w_gate, w_up, w_down):
    weights = dict(zip(NAMES, (wq, wk, wv, wo, w_gate, w_up, w_down), strict=True))

    def take(so_far, sequence):
        h, by_y = sequence
        _, back = jax.vjp(lambda w, h: layer(h, w), weights, h)
        by_weights, by_h = back(by_y)
        return jax.tree.map(lambda total, term: total + term.astype(jnp.float32), so_far, by_weights), by_h

    none_yet = {name: jnp.zeros(w.shape, jnp.float32) for name, w in weights.items()}
    by_weights, by_x = lax.scan(take, none_yet, (x, dy))
    return (by_x, *(by_weights[name].astype(jnp.bfloat16) for name in NAMES))
```

```python
import functools

import jax
import jax.numpy as jnp
from jax import lax
from jax.experimental import pallas as pl
from jax.experimental.pallas import tpu as pltpu
from jax.sharding import Mesh
from jax.sharding import PartitionSpec as P


NEG = -1e30
HIDDEN = 2 * NEG
LOG2E = 1.4426950408889634
VMEM = 58 * 2**20
HEAD = 128
THETA = 10000
HEADS = 6
KV = 2
GROUP = HEADS // KV
BLOCK = 384
SCALE = HEAD**-0.5
QW, KW = HEADS * HEAD, KV * HEAD


def _dot(a, b, ca, cb):
    return lax.dot_general(a, b, (((ca,), (cb,)), ((), ())), preferred_element_type=jnp.float32)


def _turn(t, cos, sin):
    t = t.astype(jnp.float32)
    return (t * cos + pltpu.roll(t, HEAD // 2, 1) * sin).astype(jnp.bfloat16)


def _turn_back(t, cos, sin):
    t = t.astype(jnp.bfloat16).astype(jnp.float32)
    return (t * cos + pltpu.roll(t * sin, HEAD // 2, 1)).astype(jnp.bfloat16)


def _head(h):
    return slice(h * HEAD, (h + 1) * HEAD)


def _stage(qkv, cos_ref, sin_ref, q_s, k_s):
    for half, ref in enumerate(qkv):
        for part in range(2):
            rows = slice(part * BLOCK, (part + 1) * BLOCK)
            to = slice((2 * half + part) * BLOCK, (2 * half + part + 1) * BLOCK)
            cos, sin = cos_ref[to, :], sin_ref[to, :]
            for h in range(HEADS):
                q_s[to, _head(h)] = _turn(ref[rows, _head(h)], cos, sin)
            for i in range(KV):
                k_s[to, _head(i)] = _turn(ref[rows, _head(HEADS + i)], cos, sin)


def _place(block, flip):
    at = block + flip
    return pl.multiple_of(jnp.where(at >= 4, at - 4, at) * BLOCK, BLOCK)


def _causal():
    return lax.broadcasted_iota(jnp.int32, (BLOCK, BLOCK), 1) >= lax.broadcasted_iota(jnp.int32, (BLOCK, BLOCK), 0)


def _to_half(own_ref, other_ref, at, columns, value):
    half = 2 * BLOCK

    @pl.when(at < half)
    def _():
        own_ref[pl.ds(pl.multiple_of(at, BLOCK), BLOCK), columns] = value

    @pl.when(at >= half)
    def _():
        other_ref[pl.ds(pl.multiple_of(at - half, BLOCK), BLOCK), columns] = value


def _attend_kernel(flip_ref, own_ref, other_ref, cos_ref, sin_ref, o_own_ref, o_other_ref, lse_ref, q_s, k_s, v_s, top_s, mix_s):
    flip = flip_ref[0]
    e = SCALE * LOG2E
    _stage((own_ref, other_ref), cos_ref, sin_ref, q_s, k_s)
    for half, ref in enumerate((own_ref, other_ref)):
        for i in range(KV):
            v_s[i, :HEAD, half * 2 * BLOCK : (half + 1) * 2 * BLOCK] = ref[:, _head(HEADS + KV + i)].T
    v_s[:, HEAD:, :] = jnp.ones((KV, 16, 4 * BLOCK), jnp.bfloat16)
    lse_ref[...] = jnp.zeros_like(lse_ref)

    def queries(iq, _):
        at = _place(iq, flip)
        mine = pl.ds(at, BLOCK)
        top_s[...] = jnp.full_like(top_s, NEG)
        mix_s[...] = jnp.zeros_like(mix_s)

        def block(j, masked):
            here = pl.ds(_place(j, flip), BLOCK)
            scores = [_dot(k_s[here, _head(h // GROUP)], q_s[mine, _head(h)], 1, 1) for h in range(HEADS)]
            weights, keeps = [], []
            for h, s in enumerate(scores):
                if masked:
                    s = jnp.where(_causal(), s, HIDDEN)
                old = top_s[h : h + 1, :]
                top = jnp.maximum(old, s.max(axis=0, keepdims=True))
                top_s[h : h + 1, :] = top
                weights.append(jnp.exp2((s - top) * e).astype(jnp.bfloat16))
                keeps.append(jnp.exp2((old - top) * e))
            for h, (p, keep) in enumerate(zip(weights, keeps)):
                mix_s[h] = mix_s[h] * keep + _dot(v_s[h // GROUP, :, here], p, 1, 0)

        lax.fori_loop(0, iq, lambda j, _: block(j, False), None)
        block(iq, True)
        for h in range(HEADS):
            total = mix_s[h, HEAD : HEAD + 1, :]
            out = (mix_s[h, :HEAD, :] * (1 / total)).T.astype(jnp.bfloat16)
            _to_half(o_own_ref, o_other_ref, at, _head(h), out)
            lse_ref[h : h + 1, mine] = top_s[h : h + 1, :] * SCALE + jnp.log(total)

    lax.fori_loop(0, 4, queries, None)


def _attend_bwd_kernel(flip_ref, own_ref, other_ref, cos_ref, sin_ref, o_own_ref, o_other_ref, do_own_ref, do_other_ref, lse_ref,
                       d_own_ref, d_other_ref, q_s, k_s, kt_s, v_s, do_s, dq_s, dk_s, dv_s, delta_s):
    flip = flip_ref[0]
    e = SCALE * LOG2E
    halves = ((own_ref, o_own_ref, do_own_ref), (other_ref, o_other_ref, do_other_ref))
    _stage((own_ref, other_ref), cos_ref, sin_ref, q_s, k_s)
    delta_s[...] = jnp.zeros_like(delta_s)
    for half, (ref, o_ref, do_ref) in enumerate(halves):
        to = slice(half * 2 * BLOCK, (half + 1) * 2 * BLOCK)
        v_s[to, :] = ref[:, QW + KW :]
        do_s[to, :] = do_ref[...]
        for i in range(KV):
            kt_s[i, :, to] = k_s[to, _head(i)].T
        for h in range(HEADS):
            product = do_ref[:, _head(h)].astype(jnp.float32) * o_ref[:, _head(h)].astype(jnp.float32)
            delta_s[h : h + 1, to] = product.T.sum(axis=0, keepdims=True)
    dk_s[...] = jnp.zeros_like(dk_s)
    dv_s[...] = jnp.zeros_like(dv_s)

    def queries(iq, _):
        at = _place(iq, flip)
        mine = pl.ds(at, BLOCK)
        dq_s[...] = jnp.zeros_like(dq_s)
        lses = [lse_ref[h : h + 1, mine] * LOG2E for h in range(HEADS)]
        deltas = [delta_s[h : h + 1, mine] for h in range(HEADS)]

        def block(j, masked):
            here = pl.ds(_place(j, flip), BLOCK)
            scores = [_dot(k_s[here, _head(h // GROUP)], q_s[mine, _head(h)], 1, 1) for h in range(HEADS)]
            dps = [_dot(v_s[here, _head(h // GROUP)], do_s[mine, _head(h)], 1, 1) for h in range(HEADS)]
            for i in range(KV):
                by_v = by_k = None
                for h in range(i * GROUP, (i + 1) * GROUP):
                    p = jnp.exp2(scores[h] * e - lses[h])
                    if masked:
                        p = jnp.where(_causal(), p, 0.0)
                    ds = (p * (dps[h] - deltas[h])).astype(jnp.bfloat16)
                    one = _dot(p.astype(jnp.bfloat16), do_s[mine, _head(h)], 1, 0)
                    two = _dot(ds, q_s[mine, _head(h)], 1, 0)
                    by_v, by_k = (one, two) if by_v is None else (by_v + one, by_k + two)
                    dq_s[h] += _dot(kt_s[i, :, here], ds, 1, 0)
                dv_s[here, _head(i)] += by_v
                dk_s[here, _head(i)] += by_k

        lax.fori_loop(0, iq, lambda j, _: block(j, False), None)
        block(iq, True)
        cos, sin = cos_ref[mine, :], sin_ref[mine, :]
        for h in range(HEADS):
            _to_half(d_own_ref, d_other_ref, at, _head(h), _turn_back((dq_s[h] * SCALE).T, cos, sin))

    lax.fori_loop(0, 4, queries, None)
    for half, ref in enumerate((d_own_ref, d_other_ref)):
        to = slice(half * 2 * BLOCK, (half + 1) * 2 * BLOCK)
        for i in range(KV):
            ref[:, _head(HEADS + i)] = _turn_back(dk_s[to, _head(i)] * SCALE, cos_ref[to, :], sin_ref[to, :])
            ref[:, _head(HEADS + KV + i)] = dv_s[to, _head(i)].astype(jnp.bfloat16)


def _whole(kernel, args, outs, scratch, flops, exps):
    vmem = pl.BlockSpec(memory_space=pltpu.VMEM)
    return pl.pallas_call(
        kernel,
        in_specs=[pl.BlockSpec(memory_space=pltpu.SMEM)] + [vmem] * (len(args) - 1),
        out_specs=[vmem] * len(outs),
        out_shape=outs,
        scratch_shapes=scratch,
        compiler_params=pltpu.CompilerParams(vmem_limit_bytes=VMEM),
        cost_estimate=pl.CostEstimate(flops=flops, transcendentals=exps,
                                      bytes_accessed=sum(a.size * a.dtype.itemsize for a in (*args, *outs))),
    )(*args)


def _bf16(*shape):
    return jax.ShapeDtypeStruct(shape, jnp.bfloat16)


def attend(flip, own, other, cos, sin):
    half, s = 2 * BLOCK, 4 * BLOCK
    scratch = [pltpu.VMEM((s, QW), jnp.bfloat16), pltpu.VMEM((s, KW), jnp.bfloat16), pltpu.VMEM((KV, HEAD + 16, s), jnp.bfloat16),
               pltpu.VMEM((8, BLOCK), jnp.float32), pltpu.VMEM((HEADS, HEAD + 16, BLOCK), jnp.float32)]
    return _whole(_attend_kernel, (flip, own, other, cos, sin), [_bf16(half, QW), _bf16(half, QW), jax.ShapeDtypeStruct((8, s), jnp.float32)],
                  scratch, 4 * HEADS * s * s * HEAD, HEADS * s * s)


def attend_bwd(flip, own, other, cos, sin, o_own, o_other, do_own, do_other, lse):
    half, s = 2 * BLOCK, 4 * BLOCK
    scratch = [pltpu.VMEM((s, QW), jnp.bfloat16), pltpu.VMEM((s, KW), jnp.bfloat16), pltpu.VMEM((KV, HEAD, s), jnp.bfloat16),
               pltpu.VMEM((s, KW), jnp.bfloat16), pltpu.VMEM((s, QW), jnp.bfloat16), pltpu.VMEM((HEADS, HEAD, BLOCK), jnp.float32),
               pltpu.VMEM((s, KW), jnp.float32), pltpu.VMEM((s, KW), jnp.float32), pltpu.VMEM((8, s), jnp.float32)]
    return _whole(_attend_bwd_kernel, (flip, own, other, cos, sin, o_own, o_other, do_own, do_other, lse),
                  [_bf16(half, QW + 2 * KW), _bf16(half, QW + 2 * KW)], scratch, 8 * HEADS * s * s * HEAD, HEADS * s * s)


def _gradient_kernel(cuts, a_own, a_other, *refs):
    n = len(refs) - len(cuts)
    gs, outs = refs[:n], refs[n:]
    own, other = a_own[...].T, a_other[...].T
    for (which, first, last), out in zip(cuts, outs):
        for at in range(first, last, 512):
            columns = slice(at, min(at + 512, last))
            out[:, at - first : columns.stop - first] = (
                _dot(own, gs[2 * which][:, columns], 1, 0) + _dot(other, gs[2 * which + 1][:, columns], 1, 0)
            ).astype(jnp.bfloat16)


def gradient(a, gs, cuts, rows):
    tokens, width = a[0].shape
    flat = [half for g in gs for half in g]
    outs = [_bf16(width, last - first) for _, first, last in cuts]
    block = pl.BlockSpec((tokens, rows), lambda i: (0, i))
    return pl.pallas_call(
        functools.partial(_gradient_kernel, cuts),
        grid=(width // rows,),
        in_specs=[block, block] + [pl.BlockSpec(g.shape, lambda i: (0, 0)) for g in flat],
        out_specs=[pl.BlockSpec((rows, o.shape[1]), lambda i: (i, 0)) for o in outs],
        out_shape=outs,
        compiler_params=pltpu.CompilerParams(vmem_limit_bytes=VMEM, dimension_semantics=("arbitrary",)),
        cost_estimate=pl.CostEstimate(flops=sum(4 * tokens * width * o.shape[1] for o in outs), transcendentals=0,
                                      bytes_accessed=sum(2 * v.size for v in (*a, *flat, *outs))),
    )(*a, *flat)


def matmul(a, w):
    return jnp.dot(a, w, preferred_element_type=jnp.float32).astype(jnp.bfloat16)


def matmul_t(a, w):
    return _dot(a, w, 1, 1).astype(jnp.bfloat16)


def norm_scale(h):
    wide = h.astype(jnp.float32)
    return lax.rsqrt(jnp.mean(wide**2, -1, keepdims=True) + 1e-6)


def normed(h):
    return (h.astype(jnp.float32) * norm_scale(h)).astype(jnp.bfloat16)


def norm_back(h, g):
    scale = norm_scale(h)
    unit, g = h.astype(jnp.float32) * scale, g.astype(jnp.float32)
    return scale * (g - unit * jnp.mean(g * unit, -1, keepdims=True))


def across(t):
    return lax.ppermute(t, "x", [(0, 1), (1, 0)])


def pair(t):
    return lax.all_gather(t, "c", axis=0, tiled=True)


def pair_sum(t):
    return lax.psum_scatter(t, "c", scatter_dimension=0, tiled=True)


def tie(*values):
    return lax.optimization_barrier(values)


def f32(t):
    return t.astype(jnp.float32)


def mlp(b, by_hidden, w_gate, w_up):
    gate, up = (jnp.dot(b, w, preferred_element_type=jnp.float32) for w in (w_gate, w_up))
    soft = jax.nn.sigmoid(gate)
    silu, g = gate * soft, f32(by_hidden)
    hidden = (silu * up).astype(jnp.bfloat16)
    by_up = (g * silu).astype(jnp.bfloat16)
    by_gate = (g * up * (soft * (1 + gate * (1 - soft)))).astype(jnp.bfloat16)
    return hidden, by_gate, by_up


def by_b(by_gate, by_up, w_gate, w_up):
    return (_dot(by_gate, w_gate, 1, 1) + _dot(by_up, w_up, 1, 1)).astype(jnp.bfloat16)


def step(x, dy, wq, wk, wv, wo, w_gate, w_up, w_down):
    x, dy = x[0], dy[0]
    at_x = lax.axis_index("x")
    flip = (2 * at_x).astype(jnp.int32)[None]
    place = (jnp.arange(4 * BLOCK, dtype=jnp.int32) + 2 * BLOCK * at_x) % (4 * BLOCK)
    half = HEAD // 2
    angle = place.astype(jnp.float32)[:, None] * THETA ** (-jnp.arange(half, dtype=jnp.float32) / half)
    cos, sin = jnp.cos(angle), jnp.sin(angle)
    cos, sin = jnp.concatenate([cos, cos], 1), jnp.concatenate([-sin, sin], 1)

    a = normed(x)
    a_far = across(a)
    a_own = pair(a)
    dy_own = pair(dy)
    w_qkv = jnp.concatenate([wq, wk, wv], 1)
    qkv_own = matmul(a_own, w_qkv)
    by_hidden_own = matmul_t(dy_own, w_down)
    a_far, dy_near = tie(a_far, dy)
    dy_far = across(dy_near)
    a_other = pair(a_far)
    qkv_other = matmul(a_other, w_qkv)
    o_own, o_other, lse = attend(flip, qkv_own, qkv_other, cos, sin)
    term_other = matmul(o_other, wo)
    sent, dy_far = tie(pair_sum(term_other), dy_far)
    dy_other = pair(dy_far)
    got = across(sent)
    last_o, _ = tie(o_own, term_other)
    term_own = matmul(last_o, wo)
    kept = pair_sum(term_own)
    by_hidden_other = matmul_t(dy_other, w_down)
    h = (f32(x) + (f32(kept) + f32(got))).astype(jnp.bfloat16)

    b = normed(h)
    b_far = across(b)
    b_own = pair(b)
    hidden_own, gate_own, up_own = mlp(b_own, by_hidden_own, w_gate, w_up)
    term_own = by_b(gate_own, up_own, w_gate, w_up)
    b_other = pair(b_far)
    b_other, term_own = tie(b_other, term_own)
    hidden_other, gate_other, up_other = mlp(b_other, by_hidden_other, w_gate, w_up)
    term_other = by_b(gate_other, up_other, w_gate, w_up)
    sent, term_own = tie(pair_sum(term_other), term_own)
    got = across(sent)
    kept = pair_sum(term_own)
    b_own, b_other, _ = tie(b_own, b_other, term_other)
    d_gate, d_up = gradient((b_own, b_other), ((gate_own, gate_other), (up_own, up_other)), ((0, 0, 2048), (1, 0, 2048)), 256)
    by_h = (f32(dy) + norm_back(h, f32(kept) + f32(got))).astype(jnp.bfloat16)
    hidden_own, hidden_other, _ = tie(hidden_own, hidden_other, term_other)
    (d_down,) = gradient((hidden_own, hidden_other), ((dy_own, dy_other),), ((0, 0, 3072),), 256)

    far = across(by_h)
    h_own, h_other = pair(by_h), pair(far)
    o_by_own = matmul_t(h_own, wo)
    o_by_other = matmul_t(h_other, wo)
    g_own, g_other = attend_bwd(flip, qkv_own, qkv_other, cos, sin, o_own, o_other, o_by_own, o_by_other, lse)
    term_other = matmul_t(g_other, w_qkv)
    sent = pair_sum(term_other)
    got = across(sent)
    last_g, last_o, _ = tie(g_own, o_own, term_other)
    kept = pair_sum(matmul_t(last_g, w_qkv))
    (d_o,) = gradient((last_o, o_other), ((h_own, h_other),), ((0, 0, 3072),), 256)
    d_q, d_k, d_v = gradient((a_own, a_other), ((last_g, g_other),), ((0, 0, QW), (0, QW, QW + KW), (0, QW + KW, QW + 2 * KW)), 256)
    by_x = (f32(by_h) + norm_back(x, f32(kept) + f32(got))).astype(jnp.bfloat16)
    return by_x[None], d_q, d_k, d_v, d_o, d_gate, d_up, d_down


def solution(mesh):
    split = Mesh(mesh.devices.reshape(mesh.shape["dp"], 2, 2), ("dp", "x", "c"))
    tp = ("x", "c")
    states, by_columns, by_rows = P("dp", tp, None), P(None, tp), P(tp, None)
    weights = (by_columns, by_columns, by_columns, by_rows, by_columns, by_columns, by_rows)
    own = tuple(P("dp", tp) if spec == by_columns else P(("dp", *tp), None) for spec in weights)

    return jax.shard_map(step, mesh=split, in_specs=(states, states, *weights), out_specs=(states, *own), check_vma=False)
```

```python
import functools

import jax
import jax.numpy as jnp
from jax import lax
from jax.experimental import pallas as pl
from jax.experimental.pallas import tpu as pltpu
from jax.sharding import Mesh
from jax.sharding import PartitionSpec as P


NEG = -1e30
HIDDEN = 2 * NEG
LOG2E = 1.4426950408889634
VMEM = 58 * 2**20
HEAD = 128
THETA = 10000
HEADS = 6
KV = 2
GROUP = HEADS // KV
BLOCK = 384
SCALE = HEAD**-0.5
QW, KW = HEADS * HEAD, KV * HEAD


def _dot(a, b, ca, cb):
    return lax.dot_general(a, b, (((ca,), (cb,)), ((), ())), preferred_element_type=jnp.float32)


def _turn(t, cos, sin):
    t = t.astype(jnp.float32)
    return (t * cos + pltpu.roll(t, HEAD // 2, 1) * sin).astype(jnp.bfloat16)


def _turn_back(t, cos, sin):
    t = t.astype(jnp.bfloat16).astype(jnp.float32)
    return (t * cos + pltpu.roll(t * sin, HEAD // 2, 1)).astype(jnp.bfloat16)


def _head(h):
    return slice(h * HEAD, (h + 1) * HEAD)


def _stage(qkv, cos_ref, sin_ref, q_s, k_s):
    for half, ref in enumerate(qkv):
        for part in range(2):
            rows = slice(part * BLOCK, (part + 1) * BLOCK)
            to = slice((2 * half + part) * BLOCK, (2 * half + part + 1) * BLOCK)
            cos, sin = cos_ref[to, :], sin_ref[to, :]
            for h in range(HEADS):
                q_s[to, _head(h)] = _turn(ref[rows, _head(h)], cos, sin)
            for i in range(KV):
                k_s[to, _head(i)] = _turn(ref[rows, _head(HEADS + i)], cos, sin)


def _place(block, flip):
    at = block + flip
    return pl.multiple_of(jnp.where(at >= 4, at - 4, at) * BLOCK, BLOCK)


def _causal():
    return lax.broadcasted_iota(jnp.int32, (BLOCK, BLOCK), 1) >= lax.broadcasted_iota(jnp.int32, (BLOCK, BLOCK), 0)


def _to_half(own_ref, other_ref, at, columns, value):
    half = 2 * BLOCK

    @pl.when(at < half)
    def _():
        own_ref[pl.ds(pl.multiple_of(at, BLOCK), BLOCK), columns] = value

    @pl.when(at >= half)
    def _():
        other_ref[pl.ds(pl.multiple_of(at - half, BLOCK), BLOCK), columns] = value


def _attend_kernel(flip_ref, own_ref, other_ref, cos_ref, sin_ref, o_own_ref, o_other_ref, lse_ref, q_s, k_s, v_s, top_s, mix_s):
    flip = flip_ref[0]
    e = SCALE * LOG2E
    _stage((own_ref, other_ref), cos_ref, sin_ref, q_s, k_s)
    for half, ref in enumerate((own_ref, other_ref)):
        for i in range(KV):
            v_s[i, :HEAD, half * 2 * BLOCK : (half + 1) * 2 * BLOCK] = ref[:, _head(HEADS + KV + i)].T
    v_s[:, HEAD:, :] = jnp.ones((KV, 16, 4 * BLOCK), jnp.bfloat16)
    lse_ref[...] = jnp.zeros_like(lse_ref)

    def queries(iq, _):
        at = _place(iq, flip)
        mine = pl.ds(at, BLOCK)
        top_s[...] = jnp.full_like(top_s, NEG)
        mix_s[...] = jnp.zeros_like(mix_s)

        def block(j, masked):
            here = pl.ds(_place(j, flip), BLOCK)
            scores = [_dot(k_s[here, _head(h // GROUP)], q_s[mine, _head(h)], 1, 1) for h in range(HEADS)]
            weights, keeps = [], []
            for h, s in enumerate(scores):
                if masked:
                    s = jnp.where(_causal(), s, HIDDEN)
                old = top_s[h : h + 1, :]
                top = jnp.maximum(old, s.max(axis=0, keepdims=True))
                top_s[h : h + 1, :] = top
                weights.append(jnp.exp2((s - top) * e).astype(jnp.bfloat16))
                keeps.append(jnp.exp2((old - top) * e))
            for h, (p, keep) in enumerate(zip(weights, keeps)):
                mix_s[h] = mix_s[h] * keep + _dot(v_s[h // GROUP, :, here], p, 1, 0)

        lax.fori_loop(0, iq, lambda j, _: block(j, False), None)
        block(iq, True)
        for h in range(HEADS):
            total = mix_s[h, HEAD : HEAD + 1, :]
            out = (mix_s[h, :HEAD, :] * (1 / total)).T.astype(jnp.bfloat16)
            _to_half(o_own_ref, o_other_ref, at, _head(h), out)
            lse_ref[h : h + 1, mine] = top_s[h : h + 1, :] * SCALE + jnp.log(total)

    lax.fori_loop(0, 4, queries, None)


def _attend_bwd(half, flip, own_ref, other_ref, cos_ref, sin_ref, o_ref, do_ref, lse_ref, put, dk_s, dv_s, q_s, k_s, kt_s, v_s, dq_s, delta_s):
    e = SCALE * LOG2E
    for part in range(4):
        to = slice(part * BLOCK, (part + 1) * BLOCK)
        ref, rows = (own_ref, other_ref)[part // 2], slice(part % 2 * BLOCK, (part % 2 + 1) * BLOCK)
        cos, sin = cos_ref[to, :], sin_ref[to, :]
        for i in range(KV):
            k_s[to, _head(i)] = _turn(ref[rows, _head(HEADS + i)], cos, sin)
            kt_s[i, :, to] = k_s[to, _head(i)].T
        v_s[to, :] = ref[rows, QW + KW :]
        if part // 2 == half:
            for h in range(HEADS):
                q_s[rows, _head(h)] = _turn(ref[rows, _head(h)], cos, sin)
    delta_s[...] = jnp.zeros_like(delta_s)
    for h in range(HEADS):
        product = do_ref[:, _head(h)].astype(jnp.float32) * o_ref[:, _head(h)].astype(jnp.float32)
        delta_s[h : h + 1, :] = product.T.sum(axis=0, keepdims=True)

    def queries(r, _):
        mine = pl.ds(pl.multiple_of(r * BLOCK, BLOCK), BLOCK)
        at = pl.ds(pl.multiple_of((2 * half + r) * BLOCK, BLOCK), BLOCK)
        iq = 2 * half + r + flip
        iq = jnp.where(iq >= 4, iq - 4, iq)
        dq_s[...] = jnp.zeros_like(dq_s)
        lses = [lse_ref[h : h + 1, at] * LOG2E for h in range(HEADS)]
        deltas = [delta_s[h : h + 1, mine] for h in range(HEADS)]

        def block(j, masked):
            here = pl.ds(_place(j, flip), BLOCK)
            scores = [_dot(k_s[here, _head(h // GROUP)], q_s[mine, _head(h)], 1, 1) for h in range(HEADS)]
            dps = [_dot(v_s[here, _head(h // GROUP)], do_ref[mine, _head(h)], 1, 1) for h in range(HEADS)]
            for i in range(KV):
                by_v = by_k = None
                for h in range(i * GROUP, (i + 1) * GROUP):
                    p = jnp.exp2(scores[h] * e - lses[h])
                    if masked:
                        p = jnp.where(_causal(), p, 0.0)
                    ds = (p * (dps[h] - deltas[h])).astype(jnp.bfloat16)
                    one = _dot(p.astype(jnp.bfloat16), do_ref[mine, _head(h)], 1, 0)
                    two = _dot(ds, q_s[mine, _head(h)], 1, 0)
                    by_v, by_k = (one, two) if by_v is None else (by_v + one, by_k + two)
                    dq_s[h] += _dot(kt_s[i, :, here], ds, 1, 0)
                dv_s[here, _head(i)] += by_v
                dk_s[here, _head(i)] += by_k

        lax.fori_loop(0, iq, lambda j, _: block(j, False), None)
        block(iq, True)
        cos, sin = cos_ref[at, :], sin_ref[at, :]
        for h in range(HEADS):
            put[mine, _head(h)] = _turn_back((dq_s[h] * SCALE).T, cos, sin)

    lax.fori_loop(0, 2, queries, None)


def _own_bwd_kernel(flip_ref, own_ref, other_ref, cos_ref, sin_ref, o_ref, do_ref, lse_ref, dq_ref, dk_ref, dv_ref, *scratch):
    dk_ref[...] = jnp.zeros_like(dk_ref)
    dv_ref[...] = jnp.zeros_like(dv_ref)
    _attend_bwd(0, flip_ref[0], own_ref, other_ref, cos_ref, sin_ref, o_ref, do_ref, lse_ref, dq_ref, dk_ref, dv_ref, *scratch)


def _other_bwd_kernel(flip_ref, own_ref, other_ref, cos_ref, sin_ref, o_ref, do_ref, lse_ref, dq_ref, dk_ref, dv_ref,
                      d_own_ref, d_other_ref, dk_s, dv_s, *scratch):
    dk_s[...] = dk_ref[...]
    dv_s[...] = dv_ref[...]
    d_own_ref[:, :QW] = dq_ref[...]
    _attend_bwd(1, flip_ref[0], own_ref, other_ref, cos_ref, sin_ref, o_ref, do_ref, lse_ref, d_other_ref, dk_s, dv_s, *scratch)
    for half, ref in enumerate((d_own_ref, d_other_ref)):
        to = slice(half * 2 * BLOCK, (half + 1) * 2 * BLOCK)
        for i in range(KV):
            ref[:, _head(HEADS + i)] = _turn_back(dk_s[to, _head(i)] * SCALE, cos_ref[to, :], sin_ref[to, :])
            ref[:, _head(HEADS + KV + i)] = dv_s[to, _head(i)].astype(jnp.bfloat16)


def _whole(kernel, args, outs, scratch, flops, exps, grant):
    vmem = pl.BlockSpec(memory_space=pltpu.VMEM)
    return pl.pallas_call(
        kernel,
        in_specs=[pl.BlockSpec(memory_space=pltpu.SMEM)] + [vmem] * (len(args) - 1),
        out_specs=[vmem] * len(outs),
        out_shape=outs,
        scratch_shapes=scratch,
        compiler_params=pltpu.CompilerParams(vmem_limit_bytes=grant * 2**20),
        cost_estimate=pl.CostEstimate(flops=flops, transcendentals=exps,
                                      bytes_accessed=sum(a.size * a.dtype.itemsize for a in (*args, *outs))),
    )(*args)


def _bf16(*shape):
    return jax.ShapeDtypeStruct(shape, jnp.bfloat16)


def attend(flip, own, other, cos, sin):
    half, s = 2 * BLOCK, 4 * BLOCK
    scratch = [pltpu.VMEM((s, QW), jnp.bfloat16), pltpu.VMEM((s, KW), jnp.bfloat16), pltpu.VMEM((KV, HEAD + 16, s), jnp.bfloat16),
               pltpu.VMEM((8, BLOCK), jnp.float32), pltpu.VMEM((HEADS, HEAD + 16, BLOCK), jnp.float32)]
    return _whole(_attend_kernel, (flip, own, other, cos, sin), [_bf16(half, QW), _bf16(half, QW), jax.ShapeDtypeStruct((8, s), jnp.float32)],
                  scratch, 4 * HEADS * s * s * HEAD, HEADS * s * s, 34)


def _bwd_scratch():
    half, s = 2 * BLOCK, 4 * BLOCK
    return [pltpu.VMEM((half, QW), jnp.bfloat16), pltpu.VMEM((s, KW), jnp.bfloat16), pltpu.VMEM((KV, HEAD, s), jnp.bfloat16),
            pltpu.VMEM((s, KW), jnp.bfloat16), pltpu.VMEM((HEADS, HEAD, BLOCK), jnp.float32), pltpu.VMEM((8, half), jnp.float32)]


def own_bwd(flip, own, other, cos, sin, o, by_o, lse):
    half, s = 2 * BLOCK, 4 * BLOCK
    sums = jax.ShapeDtypeStruct((s, KW), jnp.float32)
    return _whole(_own_bwd_kernel, (flip, own, other, cos, sin, o, by_o, lse), [_bf16(half, QW), sums, sums],
                  _bwd_scratch(), 4 * HEADS * s * s * HEAD, HEADS * s * half, 40)


def other_bwd(flip, own, other, cos, sin, o, by_o, lse, dq, dk, dv):
    half, s = 2 * BLOCK, 4 * BLOCK
    scratch = [pltpu.VMEM((s, KW), jnp.float32), pltpu.VMEM((s, KW), jnp.float32), *_bwd_scratch()]
    return _whole(_other_bwd_kernel, (flip, own, other, cos, sin, o, by_o, lse, dq, dk, dv), [_bf16(half, QW + 2 * KW)] * 2,
                  scratch, 4 * HEADS * s * s * HEAD, HEADS * s * half, 46)


def _gradient_kernel(cuts, a_own, a_other, *refs):
    n = len(refs) - len(cuts)
    gs, outs = refs[:n], refs[n:]
    own, other = a_own[...].T, a_other[...].T
    for (which, first, last), out in zip(cuts, outs):
        for at in range(first, last, 512):
            columns = slice(at, min(at + 512, last))
            out[:, at - first : columns.stop - first] = (
                _dot(own, gs[2 * which][:, columns], 1, 0) + _dot(other, gs[2 * which + 1][:, columns], 1, 0)
            ).astype(jnp.bfloat16)


def gradient(a, gs, cuts, rows):
    tokens, width = a[0].shape
    flat = [half for g in gs for half in g]
    outs = [_bf16(width, last - first) for _, first, last in cuts]
    block = pl.BlockSpec((tokens, rows), lambda i: (0, i))
    return pl.pallas_call(
        functools.partial(_gradient_kernel, cuts),
        grid=(width // rows,),
        in_specs=[block, block] + [pl.BlockSpec(g.shape, lambda i: (0, 0)) for g in flat],
        out_specs=[pl.BlockSpec((rows, o.shape[1]), lambda i: (i, 0)) for o in outs],
        out_shape=outs,
        compiler_params=pltpu.CompilerParams(vmem_limit_bytes=VMEM, dimension_semantics=("arbitrary",)),
        cost_estimate=pl.CostEstimate(flops=sum(4 * tokens * width * o.shape[1] for o in outs), transcendentals=0,
                                      bytes_accessed=sum(2 * v.size for v in (*a, *flat, *outs))),
    )(*a, *flat)


def matmul(a, w):
    return jnp.dot(a, w, preferred_element_type=jnp.float32).astype(jnp.bfloat16)


def matmul_t(a, w):
    return _dot(a, w, 1, 1).astype(jnp.bfloat16)


def norm_scale(h):
    wide = h.astype(jnp.float32)
    return lax.rsqrt(jnp.mean(wide**2, -1, keepdims=True) + 1e-6)


def normed(h):
    return (h.astype(jnp.float32) * norm_scale(h)).astype(jnp.bfloat16)


def f32(t):
    return t.astype(jnp.float32)


def _norm_kernel(x_ref, a_ref):
    a_ref[...] = normed(x_ref[...])


def _add_norm_kernel(x_ref, kept_ref, got_ref, h_ref, b_ref):
    h = (f32(x_ref[...]) + (f32(kept_ref[...]) + f32(got_ref[...]))).astype(jnp.bfloat16)
    h_ref[...] = h
    b_ref[...] = normed(h)


def _norm_back_kernel(h_ref, kept_ref, got_ref, past_ref, out_ref):
    g = f32(kept_ref[...]) + f32(got_ref[...])
    h = h_ref[...]
    scale = norm_scale(h)
    unit = f32(h) * scale
    back = scale * (g - unit * jnp.mean(g * unit, -1, keepdims=True))
    out_ref[...] = (f32(past_ref[...]) + back).astype(jnp.bfloat16)


def by_rows(kernel, args, results):
    tokens, d = args[0].shape
    block = pl.BlockSpec((tokens // 4, d), lambda i: (i, 0))
    return pl.pallas_call(
        kernel,
        grid=(4,),
        in_specs=[block] * len(args),
        out_specs=[block] * results,
        out_shape=[_bf16(tokens, d)] * results,
        compiler_params=pltpu.CompilerParams(vmem_limit_bytes=20 * 2**20, dimension_semantics=("arbitrary",)),
        cost_estimate=pl.CostEstimate(flops=8 * tokens * d, transcendentals=tokens, bytes_accessed=2 * tokens * d * (len(args) + results)),
    )(*args)


def across(t):
    return lax.ppermute(t, "x", [(0, 1), (1, 0)])


def partner(t):
    return lax.ppermute(t, "c", [(0, 1), (1, 0)])


def pair(t):
    return lax.all_gather(t, "c", axis=0, tiled=True)


def pair_sum(t):
    return lax.psum_scatter(t, "c", scatter_dimension=0, tiled=True)


def tie(*values):
    return lax.optimization_barrier(values)


def _mlp_kernel(first, wide, rows, core_ref, mine_ref, partners_ref, by_hidden_ref, gate_ref, up_ref, gate_rows_ref, up_rows_ref,
                hidden_ref, by_gate_ref, by_up_ref, term_ref, b_ref, b_s, by_gate_s, by_up_s):
    i = pl.program_id(0)

    @pl.when(i == 0)
    def _():
        core = core_ref[0]
        b_s[pl.ds(pl.multiple_of(core * BLOCK, BLOCK), BLOCK), :] = mine_ref[...]
        b_s[pl.ds(pl.multiple_of((1 - core) * BLOCK, BLOCK), BLOCK), :] = partners_ref[...]

    @pl.when(i < first)
    def _():
        gate, up = _dot(b_s[...], gate_ref[...], 1, 0), _dot(b_s[...], up_ref[...], 1, 0)
        soft = jax.nn.sigmoid(gate)
        silu, g = gate * soft, by_hidden_ref[...].astype(jnp.float32)
        by_up = (g * silu).astype(jnp.bfloat16)
        by_gate = (g * up * (soft * (1 + gate * (1 - soft)))).astype(jnp.bfloat16)
        hidden_ref[...] = (silu * up).astype(jnp.bfloat16)
        by_gate_ref[...] = by_gate
        by_up_ref[...] = by_up
        here = pl.ds(pl.multiple_of(i * wide, wide), wide)
        by_gate_s[:, here] = by_gate
        by_up_s[:, here] = by_up

    @pl.when(i >= first)
    def _():
        b_ref[...] = b_s[:, pl.ds(pl.multiple_of((i - first) * rows, rows), rows)]
        term_ref[...] = (_dot(by_gate_s[...], gate_rows_ref[...], 1, 1) + _dot(by_up_s[...], up_rows_ref[...], 1, 1)).astype(jnp.bfloat16)


def mlp(core, mine, partners, by_hidden, w_gate, w_up):
    tokens, d = 2 * mine.shape[0], mine.shape[1]
    units, wide, rows = w_gate.shape[1], 256, 256
    first, then = units // wide, d // rows
    at = lambda i: jnp.minimum(i, first - 1)
    later = lambda i: jnp.maximum(i - first, 0)
    some = pl.BlockSpec((tokens, wide), lambda i: (0, at(i)))
    columns = pl.BlockSpec((d, wide), lambda i: (0, at(i)))
    few_rows = pl.BlockSpec((rows, units), lambda i: (later(i), 0))
    block = pl.BlockSpec((tokens, rows), lambda i: (0, later(i)))
    part = pl.BlockSpec(mine.shape, lambda i: (0, 0))
    outs = [_bf16(tokens, units)] * 3 + [_bf16(tokens, d)] * 2
    return pl.pallas_call(
        functools.partial(_mlp_kernel, first, wide, rows),
        grid=(first + then,),
        in_specs=[pl.BlockSpec(memory_space=pltpu.SMEM), part, part, some, columns, columns, few_rows, few_rows],
        out_specs=[some, some, some, block, block],
        out_shape=outs,
        scratch_shapes=[pltpu.VMEM((tokens, d), jnp.bfloat16), pltpu.VMEM((tokens, units), jnp.bfloat16), pltpu.VMEM((tokens, units), jnp.bfloat16)],
        compiler_params=pltpu.CompilerParams(vmem_limit_bytes=50 * 2**20, dimension_semantics=("arbitrary",)),
        cost_estimate=pl.CostEstimate(flops=8 * tokens * d * units, transcendentals=tokens * units,
                                      bytes_accessed=2 * (2 * tokens * d + 4 * tokens * units + 4 * d * units)),
    )(core, mine, partners, by_hidden, w_gate, w_up, w_gate, w_up)


def _joined_kernel(transposed, last, core_ref, mine_ref, partners_ref, w_ref, out_ref, both_ref):
    core, i = core_ref[0], pl.program_id(0)
    wide = both_ref.shape[1]
    columns = pl.ds(pl.multiple_of(jnp.minimum(i, last) * wide, wide), wide)
    for at, ref in ((core, mine_ref), (1 - core, partners_ref)):
        rows = pl.ds(pl.multiple_of(at * BLOCK, BLOCK), BLOCK)
        out_ref[rows, :] = _dot(ref[...], w_ref[...], 1, 1 if transposed else 0).astype(jnp.bfloat16)
        both_ref[rows, :] = ref[:, columns]


def joined(core, mine, partners, w, transposed, copied):
    tokens, d = 2 * mine.shape[0], mine.shape[1]
    n, wide = w.shape[0 if transposed else 1], 256
    last = d // copied - 1
    part = pl.BlockSpec(mine.shape, lambda i: (0, 0))
    outs = [_bf16(tokens, n), _bf16(tokens, d)]
    return pl.pallas_call(
        functools.partial(_joined_kernel, transposed, last),
        grid=(n // wide,),
        in_specs=[pl.BlockSpec(memory_space=pltpu.SMEM), part, part,
                  pl.BlockSpec((wide, d), lambda i: (i, 0)) if transposed else pl.BlockSpec((d, wide), lambda i: (0, i))],
        out_specs=[pl.BlockSpec((tokens, wide), lambda i: (0, i)), pl.BlockSpec((tokens, copied), lambda i: (0, jnp.minimum(i, last)))],
        out_shape=outs,
        compiler_params=pltpu.CompilerParams(vmem_limit_bytes=32 * 2**20, dimension_semantics=("arbitrary",)),
        cost_estimate=pl.CostEstimate(flops=2 * tokens * d * n, transcendentals=0, bytes_accessed=2 * (2 * tokens * d + d * n + tokens * n)),
    )(core, mine, partners, w)


def step(x, dy, wq, wk, wv, wo, w_gate, w_up, w_down):
    x, dy = x[0], dy[0]
    at_x = lax.axis_index("x")
    flip = (2 * at_x).astype(jnp.int32)[None]
    place = (jnp.arange(4 * BLOCK, dtype=jnp.int32) + 2 * BLOCK * at_x) % (4 * BLOCK)
    half = HEAD // 2
    angle = place.astype(jnp.float32)[:, None] * THETA ** (-jnp.arange(half, dtype=jnp.float32) / half)
    cos, sin = jnp.cos(angle), jnp.sin(angle)
    cos, sin = jnp.concatenate([cos, cos], 1), jnp.concatenate([-sin, sin], 1)

    (a,) = by_rows(_norm_kernel, (x,), 1)
    a_far = across(a)
    a_own = pair(a)
    dy_own = pair(dy)
    w_qkv = jnp.concatenate([wq, wk, wv], 1)
    qkv_own = matmul(a_own, w_qkv)
    by_hidden_own = matmul_t(dy_own, w_down)
    a_far, dy_near = tie(a_far, dy)
    dy_far = across(dy_near)
    a_far_near = partner(a_far)
    core = lax.axis_index("c").astype(jnp.int32)[None]
    qkv_other, a_other = joined(core, a_far, a_far_near, w_qkv, False, 768)
    o_own, o_other, lse = attend(flip, qkv_own, qkv_other, cos, sin)
    term_other = matmul(o_other, wo)
    sent = pair_sum(term_other)
    sent, dy_far = tie(sent, dy_far)
    dy_other = pair(dy_far)
    got = across(sent)
    last_o, _ = tie(o_own, term_other)
    term_own = matmul(last_o, wo)
    kept = pair_sum(term_own)
    by_hidden_other = matmul_t(dy_other, w_down)
    h, b = by_rows(_add_norm_kernel, (x, kept, got), 2)

    b_far = across(b)
    b_near = partner(b)
    hidden_own, gate_own, up_own, term_own, b_own = mlp(core, b, b_near, by_hidden_own, w_gate, w_up)
    b_far_near = partner(b_far)
    b_far_near, term_own = tie(b_far_near, term_own)
    hidden_other, gate_other, up_other, term_other, b_other = mlp(core, b_far, b_far_near, by_hidden_other, w_gate, w_up)
    sent, term_own = tie(pair_sum(term_other), term_own)
    got = across(sent)
    kept = pair_sum(term_own)
    b_own, b_other, _ = tie(b_own, b_other, term_other)
    d_gate, d_up = gradient((b_own, b_other), ((gate_own, gate_other), (up_own, up_other)), ((0, 0, 2048), (1, 0, 2048)), 256)
    (by_h,) = by_rows(_norm_back_kernel, (h, kept, got, dy), 1)
    hidden_own, hidden_other, _ = tie(hidden_own, hidden_other, term_other)
    (d_down,) = gradient((hidden_own, hidden_other), ((dy_own, dy_other),), ((0, 0, 3072),), 256)

    far = across(by_h)
    h_own = pair(by_h)
    far_near = partner(far)
    o_by_own = matmul_t(h_own, wo)
    o_by_other, h_other = joined(core, far, far_near, wo, True, 1024)
    parts = own_bwd(flip, qkv_own, qkv_other, cos, sin, o_own, o_by_own, lse)
    g_own, g_other = other_bwd(flip, qkv_own, qkv_other, cos, sin, o_other, o_by_other, lse, *parts)
    term_other = matmul_t(g_other, w_qkv)
    sent = pair_sum(term_other)
    got = across(sent)
    last_g, last_o, _ = tie(g_own, o_own, term_other)
    kept = pair_sum(matmul_t(last_g, w_qkv))
    (d_o,) = gradient((last_o, o_other), ((h_own, h_other),), ((0, 0, 3072),), 256)
    d_q, d_k, d_v = gradient((a_own, a_other), ((last_g, g_other),), ((0, 0, QW), (0, QW, QW + KW), (0, QW + KW, QW + 2 * KW)), 256)
    (by_x,) = by_rows(_norm_back_kernel, (x, kept, got, by_h), 1)
    return by_x[None], d_q, d_k, d_v, d_o, d_gate, d_up, d_down


def solution(mesh):
    split = Mesh(mesh.devices.reshape(mesh.shape["dp"], 2, 2), ("dp", "x", "c"))
    tp = ("x", "c")
    states, by_columns, by_rows = P("dp", tp, None), P(None, tp), P(tp, None)
    weights = (by_columns, by_columns, by_columns, by_rows, by_columns, by_columns, by_rows)
    own = tuple(P("dp", tp) if spec == by_columns else P(("dp", *tp), None) for spec in weights)

    return jax.shard_map(step, mesh=split, in_specs=(states, states, *weights), out_specs=(states, *own), check_vma=False)
```
